32 devices in a mesh: curve: 8 (over z, x), grp: 4 (over y, core).
Axes of the slice: x: 2, y: 2, z: 4, core: 2. Of those that a mesh axis runs over, the one named last changes fastest.
Arguments:
- state: float32 [2, 512, 4, 12288], P(None, None, 'grp', 'curve'), may hold values from -6 to 6
- coef: float32 [512, 4, 12288], P(None, 'grp', 'curve'), may hold values from 0.2 to 4
- counts: int32 [4, 8], P('grp', 'curve'), may hold values from 512 to 1536, as said below
Outputs:
- smoothed: float32 [512, 4, 8192], P(None, 'grp', 'curve')
The draws below stay inside these ranges and needn't reach their ends.
Inputs may be any that keep to these rules, and one draw needn't show every extreme that they name: `counts`: each rank's count is 1024 plus the drift at its own end minus the drift at the end of the rank before it; drifts lie in -256 to 256, are zero before the first rank and at the last rank, so the curve holds 8192 blocks; in every curve one rank holds exactly 1536 blocks.
All inputs are finite; a program needn't handle non-finite values.
Results may differ from the reference program's by a relative error of at most 0.00002.
Values sent between devices are 32-bit elements; how exact they have to be, the bound alone decides.
A program may use at most 128 MiB of HBM per device.

```python
import math
import jax
import jax.numpy as jnp

AVG = 1024
HALF = 256
CAP = 1536
SWEEPS = 2
N_CURVE = 8
N_GRP = 4


def draw_counts(key, part):
    key_walk, key_peak = jax.random.split(jax.random.fold_in(key, 11))
    drift = jax.random.randint(key_walk, (N_GRP, N_CURVE), -HALF, HALF + 1)
    peak = jax.random.randint(key_peak, (N_GRP, 1), 1, N_CURVE - 1)
    column = jnp.arange(N_CURVE, dtype=jnp.int32)[None, :]
    drift = jnp.where(column == peak, HALF, jnp.where(column == peak - 1, -HALF, drift))
    drift = jnp.where(column == N_CURVE - 1, 0, drift)
    before = jnp.concatenate([jnp.zeros((N_GRP, 1), jnp.int32), drift[:, :-1]], axis=1)
    return (AVG + drift - before).astype(jnp.int32)


def block_scale(stream_key, extent, pieces, smallest, high):
    loudness, own = 1.0, jax.random.fold_in(stream_key, 6)
    for axis_at, shards_of in pieces:
        draws = jnp.exp(jax.random.uniform(jax.random.fold_in(own, axis_at), (shards_of,), jnp.float32, smallest / len(pieces), high / len(pieces)))
        loudness = loudness * jnp.repeat(draws, extent[axis_at] // shards_of).reshape([-1 if axis == axis_at else 1 for axis in range(len(extent))])
    return loudness


def gaussian(key, dims, scale, limit, pieces=(), held_as=jnp.bfloat16):
    level = block_scale(key, dims, pieces, -0.22, 0.18) if pieces else 1.0
    values = jax.random.normal(key, dims, jnp.float32) * scale * level
    return jnp.minimum(jnp.maximum(values, -limit), limit).astype(held_as)


def setup_inputs(seed: int = 0) -> dict:
    key_list = jax.random.split(jax.random.key(seed), 4)
    return {
        "state": gaussian(key_list[0], (2, 512, N_GRP, N_CURVE * CAP), 1.0, 6.0, ((2, 4), (3, 8)), jnp.float32),
        "coef": jnp.clip(jnp.exp(math.log(4.0) - 2.9957323 * jax.random.uniform(key_list[1], (512, N_GRP, N_CURVE * CAP), jnp.float32) ** block_scale(key_list[1], (512, N_GRP, N_CURVE * CAP), ((1, 4), (2, 8)), -0.2, 0.2)), 0.2, 4.0),
        "counts": draw_counts(jax.random.fold_in(key_list[3], 71), 0),
    }


def smooth(field, source, coef, left_block, right_block, low_face, high_face):
    xplus = jnp.concatenate([field[1:], jnp.concatenate([field[0:1, :, :, :, 1:], right_block[0:1]], axis=4)], axis=0)
    xminus = jnp.concatenate([jnp.concatenate([left_block[7:8], field[7:8, :, :, :, :-1]], axis=4), field[:-1]], axis=0)
    yplus = jnp.concatenate([field[:, 1:], high_face[:, None]], axis=1)
    yminus = jnp.concatenate([low_face[:, None], field[:, :-1]], axis=1)
    zeroes = jnp.zeros_like(field[:, :, 0:1])
    zplus = jnp.concatenate([field[:, :, 1:], zeroes], axis=2)
    zminus = jnp.concatenate([zeroes, field[:, :, :-1]], axis=2)
    total = xplus + xminus + yplus + yminus + zplus + zminus
    return (source + total) / (6.0 + coef)


def reference(state, coef, counts):
    prefix = jnp.cumsum(counts, axis=1) - counts
    blocks = N_CURVE * AVG
    target = jnp.arange(blocks, dtype=jnp.int32)
    owner = jnp.sum((prefix[:, None, :] <= target[None, :, None]).astype(jnp.int32), axis=2) - 1
    start = jnp.take_along_axis(prefix, owner, axis=1)
    source_col = (owner * CAP + target[None, :] - start).astype(jnp.int32)
    moved = jnp.take_along_axis(state, jnp.broadcast_to(source_col[None, None], (2, 512, N_GRP, blocks)), axis=3)
    moved_coef = jnp.take_along_axis(coef, jnp.broadcast_to(source_col[None], (512, N_GRP, blocks)), axis=2)
    field = moved[0].reshape(8, 8, 8, N_GRP, blocks)
    source = moved[1].reshape(8, 8, 8, N_GRP, blocks)
    cellcoef = moved_coef.reshape(8, 8, 8, N_GRP, blocks)
    edge = jnp.zeros((8, 8, 8, N_GRP, 1), jnp.float32)
    plane = jnp.zeros((8, 8, 1, blocks), jnp.float32)
    for sweep in range(SWEEPS):
        low_face = jnp.concatenate([plane, field[:, 7, :, :-1, :]], axis=2)
        high_face = jnp.concatenate([field[:, 0, :, 1:, :], plane], axis=2)
        field = smooth(field, source, cellcoef, edge, edge, low_face, high_face)
    return field.reshape(512, N_GRP, blocks)
```

```python
import functools

import jax
import jax.numpy as jnp
from jax import lax
from jax.experimental import pallas as pl
from jax.experimental.pallas import tpu as pltpu
from jax.sharding import PartitionSpec as P

AVG = 1024
HALF = 256
SWEEPS = 2
LANES = 128
SIDE = 8
PAD = 8
MESH = pl.DeviceIdType.MESH


def gather_counts(n, mine, every, send_sem, recv_sem):
    me = lax.axis_index("curve")
    barrier = pltpu.get_barrier_semaphore()
    for off in range(1, n):
        peer = lax.rem(me + off, n)
        pl.semaphore_signal(barrier, inc=1, device_id={"curve": peer}, device_id_type=MESH)
    pl.semaphore_wait(barrier, n - 1)
    copies = []
    for off in range(1, n):
        copies.append(
            pltpu.make_async_remote_copy(
                src_ref=mine,
                dst_ref=every.at[me],
                send_sem=send_sem.at[off],
                recv_sem=recv_sem.at[off],
                device_id={"curve": lax.rem(me + off, n)},
                device_id_type=MESH,
            )
        )
        copies[-1].start()
    every[me] = mine[...]
    for copy in copies:
        copy.wait()


def exchange(
    n, groups, cap_rows, drift, state, coef, out, raw0, raw1, raw2, mid, head, tail, from_left, from_right,
    wide, edge_out, edge_in, load_sem, send_sem, recv_sem, face_send, face_recv, out_sem,
):
    cells = SIDE * SIDE * SIDE
    own_rows = AVG // LANES
    half_rows = HALF // LANES
    rank, group = lax.axis_index("curve"), lax.axis_index("grp")
    has_left, has_right = rank > 0, rank < n - 1
    has_low, has_high = group > 0, group < groups - 1
    sides = (
        (has_left, {"curve": rank - 1}), (has_right, {"curve": rank + 1}),
        (has_low, {"grp": group - 1}), (has_high, {"grp": group + 1}),
    )
    raw = (raw0, raw1, raw2)
    loads = []
    for f, src in enumerate((state.at[0], state.at[1], coef)):
        loads.append(
            pltpu.make_async_copy(src, raw[f].at[pl.ds(PAD, cells * cap_rows)], load_sem.at[f])
        )
        loads[-1].start()
    barrier = pltpu.get_barrier_semaphore()
    for there, device in sides:
        @pl.when(there)
        def _():
            pl.semaphore_signal(barrier, inc=1, device_id=device, device_id_type=MESH)
    pl.semaphore_wait(barrier, sum(there.astype(jnp.int32) for there, _ in sides))

    drift_prev, drift_next = drift[0], drift[1]
    shift = 4 * HALF - HALF - drift_prev
    first = lax.shift_right_logical(shift, 7) - 4 * half_rows + PAD
    part = shift & (LANES - 1)
    turn = (LANES - part) & (LANES - 1)
    lane = lax.broadcasted_iota(jnp.int32, (8, LANES), 1)
    row = lax.broadcasted_iota(jnp.int32, (8, LANES), 0)
    stay = lane >= part

    def aligned(low, high):
        return pltpu.roll(jnp.where(stay, low, high), turn, 1)

    def sent(f, to_left):
        here, there, device = (
            (head, from_right, sides[0][1]) if to_left else (tail, from_left, sides[1][1])
        )
        k = f + 3 * (0 if to_left else 1)
        return pltpu.make_async_remote_copy(
            src_ref=here.at[f], dst_ref=there.at[f], send_sem=send_sem.at[k],
            recv_sem=recv_sem.at[k], device_id=device, device_id_type=MESH,
        )

    for f in range(3):
        loads[f].wait()

        @pl.loop(0, cells // 8)
        def _(g, f=f):
            base = g * (8 * cap_rows) + first
            for w in range(half_rows):
                for put, at in ((head, w), (tail, cap_rows - half_rows + w)):
                    low = raw[f][pl.ds(base + at, 8, stride=cap_rows), :]
                    high = raw[f][pl.ds(base + at + 1, 8, stride=cap_rows), :]
                    put[f, w, pl.ds(pl.multiple_of(g * 8, 8), 8), :] = aligned(low, high)

        @pl.when(has_right)
        def _():
            sent(f, False).start()

        @pl.when(has_left)
        def _():
            sent(f, True).start()

    def middle(f, x, y, z):
        base = (x * (SIDE * SIDE) + y * SIDE + z) * cap_rows + first + half_rows
        return aligned(raw[f][pl.ds(base, own_rows), :], raw[f][pl.ds(base + 1, own_rows), :])

    @pl.loop(0, SIDE)
    def _(x):
        @pl.loop(0, SIDE)
        def _(y):
            for z in range(SIDE):
                wide[0, x + 1, y + 1, z] = middle(0, x, y, z)
                mid[0, x, y, z] = middle(1, x, y, z)
                mid[1, x, y, z] = middle(2, x, y, z) + 6.0

    block = lax.broadcasted_iota(jnp.int32, (half_rows, LANES), 0) * LANES
    block = block + lax.broadcasted_iota(jnp.int32, (half_rows, LANES), 1)
    is_left = block < drift_prev
    is_right = block + (AVG - HALF) >= AVG + drift_next

    def merge(f, add, ref, lead, off):
        @pl.loop(0, SIDE)
        def _(x):
            @pl.loop(0, SIDE)
            def _(y):
                for z in range(SIDE):
                    c = x * (SIDE * SIDE) + y * SIDE + z
                    for rows, got, mask in (
                        (pl.ds(0, half_rows), from_left, is_left),
                        (pl.ds(own_rows - half_rows, half_rows), from_right, is_right),
                    ):
                        new = jnp.concatenate(
                            [got[f, w, pl.ds(c, 1), :] for w in range(half_rows)], axis=0
                        )
                        old = ref[lead, x + off, y + off, z, rows, :]
                        ref[lead, x + off, y + off, z, rows, :] = jnp.where(mask, new + add, old)

    def arrived(f):
        @pl.when(has_left)
        def _():
            sent(f, False).wait_recv()

        @pl.when(has_right)
        def _():
            sent(f, True).wait_recv()

    def faces(b):
        source = wide.at[b]
        down = pltpu.make_async_remote_copy(
            src_ref=source.at[pl.ds(1, SIDE), 1], dst_ref=source.at[pl.ds(1, SIDE), SIDE + 1],
            send_sem=face_send.at[4 * b], recv_sem=face_recv.at[4 * b],
            device_id=sides[2][1], device_id_type=MESH,
        )
        up = pltpu.make_async_remote_copy(
            src_ref=source.at[pl.ds(1, SIDE), SIDE], dst_ref=source.at[pl.ds(1, SIDE), 0],
            send_sem=face_send.at[4 * b + 1], recv_sem=face_recv.at[4 * b + 1],
            device_id=sides[3][1], device_id_type=MESH,
        )
        back = pltpu.make_async_remote_copy(
            src_ref=edge_out.at[b, 0], dst_ref=edge_in.at[b, 1],
            send_sem=face_send.at[4 * b + 2], recv_sem=face_recv.at[4 * b + 2],
            device_id=sides[0][1], device_id_type=MESH,
        )
        ahead = pltpu.make_async_remote_copy(
            src_ref=edge_out.at[b, 1], dst_ref=edge_in.at[b, 0],
            send_sem=face_send.at[4 * b + 3], recv_sem=face_recv.at[4 * b + 3],
            device_id=sides[1][1], device_id_type=MESH,
        )
        return down, up, back, ahead

    last_lane, last_spot = lane == LANES - 1, (lane == LANES - 1) & (row == own_rows - 1)
    first_lane, first_spot = lane == 0, (lane == 0) & (row == 0)

    def send_faces(b):
        down, up, back, ahead = faces(b)
        @pl.when(has_low)
        def _():
            down.start()

        @pl.when(has_high)
        def _():
            up.start()

        @pl.loop(0, SIDE)
        def _(y):
            for z in range(SIDE):
                value = pltpu.roll(wide[b, 1, y + 1, z], LANES - 1, 1)
                carry = pltpu.roll(value, own_rows - 1, 0)
                wide[b, SIDE + 1, y + 1, z] = jnp.where(last_lane, carry, value)
                edge_out[b, 0, y, pl.ds(z, 1), :] = carry[own_rows - 1 : own_rows]
                value = pltpu.roll(wide[b, SIDE, y + 1, z], 1, 1)
                carry = pltpu.roll(value, 1, 0)
                wide[b, 0, y + 1, z] = jnp.where(first_lane, carry, value)
                edge_out[b, 1, y, pl.ds(z, 1), :] = carry[0:1]

        @pl.when(has_left)
        def _():
            back.start()

        @pl.when(has_right)
        def _():
            ahead.start()

        for there, at in ((has_low, 0), (has_high, SIDE + 1)):
            @pl.when(jnp.logical_not(there))
            def _():
                @pl.loop(0, SIDE)
                def _(x):
                    wide[b, x + 1, at] = jnp.zeros((SIDE, own_rows, LANES), jnp.float32)

        for there, at in ((has_left, 0), (has_right, 1)):
            @pl.when(jnp.logical_not(there))
            def _():
                edge_in[b, at] = jnp.zeros((SIDE, SIDE, LANES), jnp.float32)

    def take_faces(b):
        down, up, back, ahead = faces(b)
        @pl.when(has_left)
        def _():
            ahead.wait_recv()

        @pl.when(has_right)
        def _():
            back.wait_recv()

        @pl.loop(0, SIDE)
        def _(y):
            for z in range(SIDE):
                got = jnp.broadcast_to(edge_in[b, 1, y, pl.ds(z, 1), :], (8, LANES))
                old = wide[b, SIDE + 1, y + 1, z]
                wide[b, SIDE + 1, y + 1, z] = jnp.where(last_spot, got, old)
                got = jnp.broadcast_to(edge_in[b, 0, y, pl.ds(z, 1), :], (8, LANES))
                old = wide[b, 0, y + 1, z]
                wide[b, 0, y + 1, z] = jnp.where(first_spot, got, old)

        @pl.when(has_low)
        def _():
            up.wait_recv()

        @pl.when(has_high)
        def _():
            down.wait_recv()

    def sweep(b, put):
        @pl.loop(0, SIDE)
        def _(x):
            @pl.loop(0, SIDE)
            def _(y):
                line = [wide[b, x + 1, y + 1, z] for z in range(SIDE)]
                for z in range(SIDE):
                    total = wide[b, x + 2, y + 1, z] + wide[b, x, y + 1, z]
                    total = total + (wide[b, x + 1, y + 2, z] + wide[b, x + 1, y, z])
                    if z + 1 < SIDE:
                        total = total + line[z + 1]
                    if z > 0:
                        total = total + line[z - 1]
                    put(x, y, z, (mid[0, x, y, z] + total) / mid[1, x, y, z])

    arrived(0)
    merge(0, 0.0, wide, 0, 1)
    send_faces(0)
    arrived(1)
    merge(1, 0.0, mid, 0, 0)
    arrived(2)
    merge(2, 6.0, mid, 1, 0)

    def to_wide(b):
        def put(x, y, z, value):
            wide[b, x + 1, y + 1, z] = value
        return put

    def to_mid(x, y, z, value):
        mid[0, x, y, z] = value

    for b in range(SWEEPS):
        take_faces(b)
        if b + 1 < SWEEPS:
            sweep(b, to_wide(b + 1))
            send_faces(b + 1)
        else:
            sweep(b, to_mid)
    done = pltpu.make_async_copy(mid.at[0], out, out_sem)
    done.start()
    for b in range(SWEEPS):
        for (there, _), copy in zip((sides[2], sides[3], sides[0], sides[1]), faces(b)):
            @pl.when(there)
            def _():
                copy.wait_send()
    for f in range(3):
        @pl.when(has_right)
        def _():
            sent(f, False).wait_send()

        @pl.when(has_left)
        def _():
            sent(f, True).wait_send()
    done.wait()


def local(state, coef, counts):
    n, groups = lax.axis_size("curve"), lax.axis_size("grp")
    rank = lax.axis_index("curve")
    cells, cap = state.shape[1], state.shape[3]
    cap_rows, own_rows, half_rows = cap // LANES, AVG // LANES, HALF // LANES
    mine = jnp.broadcast_to(counts, (8, LANES))
    every = pl.pallas_call(
        functools.partial(gather_counts, n),
        out_shape=jax.ShapeDtypeStruct((n, 8, LANES), jnp.int32),
        in_specs=[pl.BlockSpec(memory_space=pltpu.VMEM)],
        out_specs=pl.BlockSpec(memory_space=pltpu.VMEM),
        scratch_shapes=[pltpu.SemaphoreType.DMA((n,)), pltpu.SemaphoreType.DMA((n,))],
        compiler_params=pltpu.CompilerParams(collective_id=0, has_side_effects=True),
    )(mine)[:, 0, 0]
    order = jnp.arange(n, dtype=jnp.int32)
    before = jnp.sum(jnp.where(order < rank, every, 0))
    drift_prev = before - rank * AVG
    drift = jnp.stack([drift_prev, drift_prev + counts[0, 0] - AVG])
    f32 = jnp.float32
    out = pl.pallas_call(
        functools.partial(exchange, n, groups, cap_rows),
        out_shape=jax.ShapeDtypeStruct((SIDE, SIDE, SIDE, own_rows, LANES), f32),
        in_specs=[
            pl.BlockSpec(memory_space=pltpu.SMEM),
            pl.BlockSpec(memory_space=pl.ANY),
            pl.BlockSpec(memory_space=pl.ANY),
        ],
        out_specs=pl.BlockSpec(memory_space=pl.ANY),
        scratch_shapes=[
            *[pltpu.VMEM((cells * cap_rows + 2 * PAD, LANES), f32) for _ in range(3)],
            pltpu.VMEM((2, SIDE, SIDE, SIDE, own_rows, LANES), f32),
            pltpu.VMEM((3, half_rows, cells, LANES), f32),
            pltpu.VMEM((3, half_rows, cells, LANES), f32),
            pltpu.VMEM((3, half_rows, cells, LANES), f32),
            pltpu.VMEM((3, half_rows, cells, LANES), f32),
            pltpu.VMEM((SWEEPS, SIDE + 2, SIDE + 2, SIDE, own_rows, LANES), f32),
            pltpu.VMEM((SWEEPS, 2, SIDE, SIDE, LANES), f32),
            pltpu.VMEM((SWEEPS, 2, SIDE, SIDE, LANES), f32),
            pltpu.SemaphoreType.DMA((3,)),
            pltpu.SemaphoreType.DMA((6,)),
            pltpu.SemaphoreType.DMA((6,)),
            pltpu.SemaphoreType.DMA((4 * SWEEPS,)),
            pltpu.SemaphoreType.DMA((4 * SWEEPS,)),
            pltpu.SemaphoreType.DMA,
        ],
        compiler_params=pltpu.CompilerParams(
            collective_id=1, has_side_effects=True, vmem_limit_bytes=48 * 1024 * 1024
        ),
    )(drift, state.reshape(2, cells * cap_rows, LANES), coef.reshape(cells * cap_rows, LANES))
    return out.reshape(cells, 1, AVG)


def solution(mesh):
    placed = (P(None, None, "grp", "curve"), P(None, "grp", "curve"), P("grp", "curve"))
    return jax.shard_map(
        local, mesh=mesh, in_specs=placed, out_specs=P(None, "grp", "curve"), check_vma=False
    )
```

```python
import functools

import jax
import jax.numpy as jnp
from jax import lax
from jax.experimental import pallas as pl
from jax.experimental.pallas import tpu as pltpu
from jax.sharding import PartitionSpec as P

AVG = 1024
HALF = 256
LANES = 128
SIDE = 8
PAD = 8
WIDE = 16
LEAD = 4
MESH = pl.DeviceIdType.MESH


def gather_counts(n, mine, ghost_out, every, ghost_in, send_sem, recv_sem, ghost_send, ghost_recv):
    me = lax.axis_index("curve")
    barrier = pltpu.get_barrier_semaphore()
    for off in range(1, n):
        peer = lax.rem(me + off, n)
        pl.semaphore_signal(barrier, inc=1, device_id={"curve": peer}, device_id_type=MESH)
    pl.semaphore_wait(barrier, n - 1)
    has_left, has_right = me > 0, me < n - 1
    ghosts = []
    for side, device in ((0, {"curve": me - 1}), (1, {"curve": me + 1})):
        ghosts.append(
            pltpu.make_async_remote_copy(
                src_ref=ghost_out.at[side], dst_ref=ghost_in.at[1 - side],
                send_sem=ghost_send.at[side], recv_sem=ghost_recv.at[side],
                device_id=device, device_id_type=MESH,
            )
        )
    for there, copy in zip((has_left, has_right), ghosts):
        @pl.when(there)
        def _():
            copy.start()
    copies = []
    for off in range(1, n):
        copies.append(
            pltpu.make_async_remote_copy(
                src_ref=mine,
                dst_ref=every.at[me],
                send_sem=send_sem.at[off],
                recv_sem=recv_sem.at[off],
                device_id={"curve": lax.rem(me + off, n)},
                device_id_type=MESH,
            )
        )
        copies[-1].start()
    every[me] = mine[...]
    for there, at in ((has_left, 0), (has_right, 1)):
        @pl.when(jnp.logical_not(there))
        def _():
            ghost_in[at] = jnp.zeros(ghost_in.shape[1:], jnp.float32)
    for copy in copies:
        copy.wait()
    for there, back, forth in ((has_left, 1, 0), (has_right, 0, 1)):
        @pl.when(there)
        def _():
            ghosts[back].wait_recv()
            ghosts[forth].wait_send()


def exchange(
    n, groups, cap_rows, drift, ghost, state, coef, out, raw0, raw1, raw2, wide0, wide1, source,
    inverse, out0, out1, out2, out3, in0, in1, in2, in3, face0, face1, near0, near1, inv, first_fix,
    second_fix, result, edge_out, edge_in, load_sem, send_sem, recv_sem, face_send, face_recv, out_sem,
):
    cells = SIDE * SIDE * SIDE
    own_rows = AVG // LANES
    half_rows = HALF // LANES
    rank, group = lax.axis_index("curve"), lax.axis_index("grp")
    has_left, has_right = rank > 0, rank < n - 1
    has_low, has_high = group > 0, group < groups - 1
    sides = (
        (has_left, {"curve": rank - 1}), (has_right, {"curve": rank + 1}),
        (has_low, {"grp": group - 1}), (has_high, {"grp": group + 1}),
    )
    raw = (raw0, raw1, raw2)
    loads = []
    for f, src in ((0, state.at[0]), (2, coef), (1, state.at[1])):
        load = pltpu.make_async_copy(src, raw[f].at[pl.ds(PAD, cells * cap_rows)], load_sem.at[f])
        load.start()
        loads.append((f, load))
    loads = dict(loads)
    barrier = pltpu.get_barrier_semaphore()
    for there, device in sides:
        @pl.when(there)
        def _():
            pl.semaphore_signal(barrier, inc=1, device_id=device, device_id_type=MESH)
    pl.semaphore_wait(barrier, sum(there.astype(jnp.int32) for there, _ in sides))

    drift_prev, drift_next = drift[0], drift[1]
    shift = 8 * LANES - LEAD * LANES - drift_prev
    first = lax.shift_right_logical(shift, 7) - 8 + PAD
    part = shift & (LANES - 1)
    turn = (LANES - part) & (LANES - 1)
    lane = lax.broadcasted_iota(jnp.int32, (8, LANES), 1)
    row = lax.broadcasted_iota(jnp.int32, (8, LANES), 0)
    stay = lane >= part
    low_rows, high_rows = pl.ds(0, 8), pl.ds(8, 8)
    own = pl.ds(LEAD, own_rows)
    to_left, to_right = 2, LEAD + own_rows - 8
    zero = jnp.zeros((8, LANES), jnp.float32)

    def each(fn):
        @pl.loop(0, SIDE)
        def _(x):
            @pl.loop(0, SIDE)
            def _(y):
                fn(x, y)

    def aligned(f, x, y, z, half):
        base = (x * (SIDE * SIDE) + y * SIDE + z) * cap_rows + first + 8 * half
        low, high = raw[f][pl.ds(base, 8), :], raw[f][pl.ds(base + 1, 8), :]
        return pltpu.roll(jnp.where(stay, low, high), turn, 1)

    kinds = ((out0, in0), (out1, in1), (out2, in2), (out3, in3))

    def sent(kind, side):
        return pltpu.make_async_remote_copy(
            src_ref=kinds[kind][0].at[side], dst_ref=kinds[kind][1].at[1 - side],
            send_sem=send_sem.at[2 * kind + side], recv_sem=recv_sem.at[2 * kind + side],
            device_id=sides[side][1], device_id_type=MESH,
        )

    def send(kind):
        @pl.when(has_right)
        def _():
            sent(kind, 1).start()

        @pl.when(has_left)
        def _():
            sent(kind, 0).start()

    def arrived(kind):
        @pl.when(has_left)
        def _():
            sent(kind, 1).wait_recv()

        @pl.when(has_right)
        def _():
            sent(kind, 0).wait_recv()

    def pack(put, get, planes):
        @pl.loop(0, SIDE)
        def _(x):
            for p, y in enumerate(planes):
                for z in range(SIDE):
                    put[0, p, x, z] = get(x, y, z, pl.ds(to_left, half_rows))
                    put[1, p, x, z] = get(x, y, z, pl.ds(8 + to_right, half_rows))

    outer, near_outer = (0, SIDE - 1), (0, 1, SIDE - 2, SIDE - 1)
    loads[0].wait()

    def step(x, y):
        for z in range(SIDE):
            wide0[x + 1, y + 1, z, low_rows, :] = aligned(0, x, y, z, 0)
            wide0[x + 1, y + 1, z, high_rows, :] = aligned(0, x, y, z, 1)
    each(step)
    pack(out0, lambda x, y, z, rows: wide0[x + 1, y + 1, z, rows, :], outer)
    send(0)
    loads[2].wait()

    def step(x, y):
        for z in range(SIDE):
            inverse[x, y, z, low_rows, :] = 1.0 / (aligned(2, x, y, z, 0) + 6.0)
            inverse[x, y, z, high_rows, :] = 1.0 / (aligned(2, x, y, z, 1) + 6.0)
    each(step)
    pack(out1, lambda x, y, z, rows: inverse[x, y, z, rows, :], near_outer)
    send(1)
    loads[1].wait()

    def step(x, y):
        for z in range(SIDE):
            source[x, y, z, low_rows, :] = aligned(1, x, y, z, 0)
            source[x, y, z, high_rows, :] = aligned(1, x, y, z, 1)
    each(step)

    block = row * LANES + lane - LEAD * LANES
    for side, at, planes in (
        (0, drift_prev - 1, ((wide0, 1, SIDE - 1), (wide0, 1, SIDE), (source, 0, SIDE - 1), (inverse, 0, SIDE - 1))),
        (1, AVG + drift_next, ((wide0, 1, 2), (wide0, 1, 1), (source, 0, 0), (inverse, 0, 0))),
    ):
        here = (block == at, block + 8 * LANES == at)
        for p, (ref, off, x) in enumerate(planes):
            @pl.loop(0, SIDE)
            def _(y):
                for z in range(SIDE):
                    value = ghost[side * 4 * SIDE * SIDE + p * SIDE * SIDE + y * SIDE + z]
                    for half, rows in enumerate((low_rows, high_rows)):
                        old = ref[x, y + off, z, rows, :]
                        ref[x, y + off, z, rows, :] = jnp.where(here[half], value, old)

    def borders(ref):
        @pl.loop(0, SIDE)
        def _(y):
            for z in range(SIDE):
                turned = [pltpu.roll(ref[1, y + 1, z, rows, :], LANES - 1, 1) for rows in (low_rows, high_rows)]
                carry = [pltpu.roll(value, 7, 0) for value in turned]
                carry[0] = jnp.where(row == 7, carry[1], carry[0])
                for half, rows in enumerate((low_rows, high_rows)):
                    ref[SIDE + 1, y + 1, z, rows, :] = jnp.where(lane == LANES - 1, carry[half], turned[half])
                turned = [pltpu.roll(ref[SIDE, y + 1, z, rows, :], 1, 1) for rows in (low_rows, high_rows)]
                carry = [pltpu.roll(value, 1, 0) for value in turned]
                carry[1] = jnp.where(row == 0, carry[0], carry[1])
                for half, rows in enumerate((low_rows, high_rows)):
                    ref[0, y + 1, z, rows, :] = jnp.where(lane == 0, carry[half], turned[half])

        @pl.loop(0, SIDE)
        def _(x):
            for at in (0, SIDE + 1):
                ref[x + 1, at] = jnp.zeros((SIDE, WIDE, LANES), jnp.float32)

    def sweep(ref, put):
        def step(x, y):
            for rows in (low_rows, high_rows):
                line = [ref[x + 1, y + 1, z, rows, :] for z in range(SIDE)]
                for z in range(SIDE):
                    total = ref[x + 2, y + 1, z, rows, :] + ref[x, y + 1, z, rows, :]
                    total = total + (ref[x + 1, y + 2, z, rows, :] + ref[x + 1, y, z, rows, :])
                    if z + 1 < SIDE:
                        total = total + line[z + 1]
                    if z > 0:
                        total = total + line[z - 1]
                    value = (source[x, y, z, rows, :] + total) * inverse[x, y, z, rows, :]
                    put(x, y, z, rows, value)
        each(step)

    def put(x, y, z, rows, value):
        wide1[x + 1, y + 1, z, rows, :] = value
    borders(wide0)
    sweep(wide0, put)
    pack(out2, lambda x, y, z, rows: wide1[x + 1, y + 1, z, rows, :], outer)
    send(2)

    def put(x, y, z, rows, value):
        if rows is low_rows:
            result[x, y, z, pl.ds(0, 8 - LEAD), :] = value[LEAD:]
            out3[0, x, y, z] = value[to_left : to_left + half_rows]
        else:
            result[x, y, z, pl.ds(8 - LEAD, own_rows - 8 + LEAD), :] = value[:to_right]
            out3[1, x, y, z] = value[to_right : to_right + half_rows]
    borders(wide1)
    sweep(wide1, put)

    spot = lax.broadcasted_iota(jnp.int32, (half_rows, LANES), 0) * LANES
    spot = spot + lax.broadcasted_iota(jnp.int32, (half_rows, LANES), 1)
    is_left = spot < drift_prev
    is_right = spot + (AVG - HALF) >= AVG + drift_next

    def merge(kind, to, get, planes):
        got = kinds[kind][1]
        @pl.loop(0, SIDE)
        def _(x):
            for p, y in enumerate(planes):
                for z in range(SIDE):
                    mine = get(x, y, z)
                    to[p, x, z] = mine
                    to[p, x, z, pl.ds(0, half_rows), :] = jnp.where(is_left, got[0, p, x, z], mine[:half_rows])
                    to[p, x, z, pl.ds(own_rows - half_rows, half_rows), :] = jnp.where(
                        is_right, got[1, p, x, z], mine[own_rows - half_rows :]
                    )

    def faces(b):
        face, near = ((face0, near0), (face1, near1))[b]
        down = pltpu.make_async_remote_copy(
            src_ref=face.at[0], dst_ref=near.at[1], send_sem=face_send.at[2 * b],
            recv_sem=face_recv.at[2 * b], device_id=sides[2][1], device_id_type=MESH,
        )
        up = pltpu.make_async_remote_copy(
            src_ref=face.at[1], dst_ref=near.at[0], send_sem=face_send.at[2 * b + 1],
            recv_sem=face_recv.at[2 * b + 1], device_id=sides[3][1], device_id_type=MESH,
        )
        return down, up

    def send_faces(b):
        for (there, _), copy in zip(sides[2:], faces(b)):
            @pl.when(there)
            def _():
                copy.start()
        for (there, _), at in zip(sides[2:], (0, 1)):
            @pl.when(jnp.logical_not(there))
            def _():
                @pl.loop(0, SIDE)
                def _(x):
                    (near0, near1)[b][at, x] = jnp.zeros((SIDE, own_rows, LANES), jnp.float32)

    def take_faces(b):
        down, up = faces(b)
        @pl.when(has_low)
        def _():
            up.wait_recv()

        @pl.when(has_high)
        def _():
            down.wait_recv()

    arrived(0)
    merge(0, face0, lambda x, y, z: wide0[x + 1, y + 1, z, own, :], outer)
    send_faces(0)
    arrived(1)
    merge(1, inv, lambda x, y, z: inverse[x, y, z, own, :], near_outer)
    take_faces(0)

    @pl.loop(0, SIDE)
    def _(x):
        for p, at, inner in ((0, 0, 1), (1, 3, 2)):
            for z in range(SIDE):
                fix = near0[p, x, z] * inv[at, x, z]
                first_fix[p, x + 1, z] = fix
                second_fix[inner, x, z] = fix * inv[inner, x, z]

    def edges(side):
        return pltpu.make_async_remote_copy(
            src_ref=edge_out.at[side], dst_ref=edge_in.at[1 - side],
            send_sem=face_send.at[4 + side], recv_sem=face_recv.at[4 + side],
            device_id=sides[side][1], device_id_type=MESH,
        )

    for p in range(2):
        for z in range(SIDE):
            value = pltpu.roll(first_fix[p, 1, z], LANES - 1, 1)
            carry = pltpu.roll(value, own_rows - 1, 0)
            first_fix[p, SIDE + 1, z] = jnp.where(lane == LANES - 1, carry, value)
            edge_out[0, p, pl.ds(z, 1), :] = carry[own_rows - 1 : own_rows]
            value = pltpu.roll(first_fix[p, SIDE, z], 1, 1)
            carry = pltpu.roll(value, 1, 0)
            first_fix[p, 0, z] = jnp.where(lane == 0, carry, value)
            edge_out[1, p, pl.ds(z, 1), :] = carry[0:1]
    for side in range(2):
        @pl.when(sides[side][0])
        def _():
            edges(side).start()

        @pl.when(jnp.logical_not(sides[side][0]))
        def _():
            edge_in[side] = jnp.zeros((2, SIDE, LANES), jnp.float32)
    send(3)
    arrived(2)
    merge(2, face1, lambda x, y, z: wide1[x + 1, y + 1, z, own, :], outer)

    @pl.loop(0, SIDE)
    def _(x):
        for p in range(2):
            for z in range(SIDE):
                face1[p, x, z] = face1[p, x, z] + first_fix[p, x + 1, z]
    send_faces(1)
    for side in range(2):
        @pl.when(sides[side][0])
        def _():
            edges(1 - side).wait_recv()
    last_spot = (lane == LANES - 1) & (row == own_rows - 1)
    first_spot = (lane == 0) & (row == 0)
    for p in range(2):
        for z in range(SIDE):
            got = jnp.broadcast_to(edge_in[1, p, pl.ds(z, 1), :], (8, LANES))
            first_fix[p, SIDE + 1, z] = jnp.where(last_spot, got, first_fix[p, SIDE + 1, z])
            got = jnp.broadcast_to(edge_in[0, p, pl.ds(z, 1), :], (8, LANES))
            first_fix[p, 0, z] = jnp.where(first_spot, got, first_fix[p, 0, z])
    take_faces(1)

    @pl.loop(0, SIDE)
    def _(x):
        for p, at in ((0, 0), (1, 3)):
            for z in range(SIDE):
                total = near1[p, x, z] + (first_fix[p, x, z] + first_fix[p, x + 2, z])
                if z + 1 < SIDE:
                    total = total + first_fix[p, x + 1, z + 1]
                if z > 0:
                    total = total + first_fix[p, x + 1, z - 1]
                second_fix[at, x, z] = total * inv[at, x, z]

    arrived(3)
    lo, hi = pl.ds(0, half_rows), pl.ds(own_rows - half_rows, half_rows)

    def step(x, y):
        for z in range(SIDE):
            for side, rows, mask in ((0, lo, is_left), (1, hi, is_right)):
                old = result[x, y, z, rows, :]
                result[x, y, z, rows, :] = jnp.where(mask, in3[side, x, y, z], old)
    each(step)

    @pl.loop(0, SIDE)
    def _(x):
        for p, y in enumerate(near_outer):
            for z in range(SIDE):
                result[x, y, z] = result[x, y, z] + second_fix[p, x, z]
    done = pltpu.make_async_copy(result, out, out_sem)
    done.start()
    for b in range(2):
        for (there, _), copy in zip(sides[2:], faces(b)):
            @pl.when(there)
            def _():
                copy.wait_send()
    for side in range(2):
        @pl.when(sides[side][0])
        def _():
            edges(side).wait_send()
            for kind in range(4):
                sent(kind, side).wait_send()
    done.wait()


def local(state, coef, counts):
    n, groups = lax.axis_size("curve"), lax.axis_size("grp")
    rank = lax.axis_index("curve")
    cells, cap = state.shape[1], state.shape[3]
    cap_rows, own_rows, half_rows = cap // LANES, AVG // LANES, HALF // LANES
    plane = SIDE * SIDE
    held = counts[0, 0]
    f32 = jnp.float32

    def end_block(at, outer, near):
        cell = lax.dynamic_slice_in_dim(state, at, 1, 3)[:, :, 0, 0].reshape(2, SIDE, plane)
        scale = lax.dynamic_slice_in_dim(coef, at, 1, 2)[:, 0, 0].reshape(SIDE, plane)
        return jnp.stack([cell[0, outer], cell[0, near], cell[1, near], 1.0 / (6.0 + scale[near])])

    ends = jnp.stack([end_block(0, 1, 0), end_block(held - 1, SIDE - 2, SIDE - 1)])
    ends = ends.reshape(2, 4 * plane // LANES, LANES)
    mine = jnp.broadcast_to(counts, (8, LANES))
    vmem, hbm, smem = (pl.BlockSpec(memory_space=m) for m in (pltpu.VMEM, pl.ANY, pltpu.SMEM))
    every, ghost = pl.pallas_call(
        functools.partial(gather_counts, n),
        out_shape=(jax.ShapeDtypeStruct((n, 8, LANES), jnp.int32), jax.ShapeDtypeStruct(ends.shape, f32)),
        in_specs=[vmem, vmem],
        out_specs=(vmem, vmem),
        scratch_shapes=[pltpu.SemaphoreType.DMA((k,)) for k in (n, n, 2, 2)],
        compiler_params=pltpu.CompilerParams(collective_id=0, has_side_effects=True),
    )(mine, ends)
    order = jnp.arange(n, dtype=jnp.int32)
    before = jnp.sum(jnp.where(order < rank, every[:, 0, 0], 0))
    drift_prev = before - rank * AVG
    drift = jnp.stack([drift_prev, drift_prev + held - AVG])
    side = (SIDE, SIDE)
    packed = [(2, 2) + side, (2, 4) + side, (2, 2) + side, (2, SIDE) + side]
    packed = [shape + (half_rows, LANES) for shape in packed]
    own = (own_rows, LANES)
    shapes = [(cells * cap_rows + 2 * PAD, LANES)] * 3
    shapes += [(SIDE + 2, SIDE + 2, SIDE, WIDE, LANES)] * 2 + [side + (SIDE, WIDE, LANES)] * 2
    shapes += packed + packed + [(2,) + side + own] * 4
    shapes += [(4,) + side + own, (2, SIDE + 2, SIDE) + own, (4,) + side + own, side + (SIDE,) + own]
    shapes += [(2, 2, SIDE, LANES)] * 2
    out = pl.pallas_call(
        functools.partial(exchange, n, groups, cap_rows),
        out_shape=jax.ShapeDtypeStruct((SIDE, SIDE, SIDE, own_rows, LANES), f32),
        in_specs=[smem, smem, hbm, hbm],
        out_specs=hbm,
        scratch_shapes=[pltpu.VMEM(shape, f32) for shape in shapes]
        + [pltpu.SemaphoreType.DMA((k,)) for k in (3, 8, 8, 6, 6)]
        + [pltpu.SemaphoreType.DMA],
        compiler_params=pltpu.CompilerParams(
            collective_id=1, has_side_effects=True, vmem_limit_bytes=56 * 1024 * 1024
        ),
    )(
        drift, ghost.reshape(-1), state.reshape(2, cells * cap_rows, LANES),
        coef.reshape(cells * cap_rows, LANES),
    )
    return out.reshape(cells, 1, AVG)


def solution(mesh):
    placed = (P(None, None, "grp", "curve"), P(None, "grp", "curve"), P("grp", "curve"))
    return jax.shard_map(
        local, mesh=mesh, in_specs=placed, out_specs=P(None, "grp", "curve"), check_vma=False
    )
```

```python
import functools

import jax
import jax.numpy as jnp
from jax import lax
from jax.experimental import pallas as pl
from jax.experimental.pallas import tpu as pltpu
from jax.sharding import PartitionSpec as P

AVG = 1024
HALF = 256
LANES = 128
SIDE = 8
PAD = 8
WIDE = 16
LEAD = 4
MESH = pl.DeviceIdType.MESH


def exchange(
    n, groups, cap_rows, counts, mine, state, coef, out, every, every_s, ends, met, ghost, raw0, raw1, raw2, wide0, wide1, source,
    inverse, out0, out1, out2, out3, in0, in1, in2, in3, face0, face1, near0, near1, inv, first_fix,
    second_fix, result, edge_out, edge_in, count_send, count_recv, end_send, end_recv, local_sem, load_sem, send_sem, recv_sem, face_send, face_recv, out_sem,
):
    cells = SIDE * SIDE * SIDE
    own_rows = AVG // LANES
    half_rows = HALF // LANES
    rank, group = lax.axis_index("curve"), lax.axis_index("grp")
    has_left, has_right = rank > 0, rank < n - 1
    has_low, has_high = group > 0, group < groups - 1
    sides = (
        (has_left, {"curve": rank - 1}), (has_right, {"curve": rank + 1}),
        (has_low, {"grp": group - 1}), (has_high, {"grp": group + 1}),
    )
    raw = (raw0, raw1, raw2)
    loads = []
    for f, src in ((0, state.at[0]), (2, coef), (1, state.at[1])):
        load = pltpu.make_async_copy(src, raw[f].at[pl.ds(PAD, cells * cap_rows)], load_sem.at[f])
        load.start()
        loads.append((f, load))
    loads = dict(loads)
    barrier = pltpu.get_barrier_semaphore()
    for there, device in sides:
        @pl.when(there)
        def _():
            pl.semaphore_signal(barrier, inc=1, device_id=device, device_id_type=MESH)
    for off in range(2, n - 1):
        peer = lax.rem(rank + off, n)
        pl.semaphore_signal(barrier, inc=1, device_id={"curve": peer}, device_id_type=MESH)
    for there, peer in ((has_left, n - 1), (has_right, 0)):
        @pl.when(jnp.logical_not(there))
        def _():
            pl.semaphore_signal(barrier, inc=1, device_id={"curve": peer}, device_id_type=MESH)
    pl.semaphore_wait(barrier, n - 1 + has_low.astype(jnp.int32) + has_high.astype(jnp.int32))

    tallies = []
    for off in range(1, n):
        tallies.append(
            pltpu.make_async_remote_copy(
                src_ref=mine, dst_ref=every.at[rank], send_sem=count_send.at[off],
                recv_sem=count_recv.at[off], device_id={"curve": lax.rem(rank + off, n)},
                device_id_type=MESH,
            )
        )
        tallies[-1].start()
    keep = pltpu.make_async_copy(mine, every.at[rank], local_sem.at[0])
    keep.start()
    lane = lax.broadcasted_iota(jnp.int32, (8, LANES), 1)
    row = lax.broadcasted_iota(jnp.int32, (8, LANES), 0)
    held = counts[0, 0]
    last = jnp.clip(held - 1, 0, cap_rows * LANES - 1)
    last_row = lax.shift_right_logical(last, 7)
    last_turn = (LANES - (last & (LANES - 1))) & (LANES - 1)
    for f in range(3):
        loads[f].wait()
    for side, at, turn, outer_x, near_x in ((0, 0, 0, 1, 0), (1, last_row, last_turn, SIDE - 2, SIDE - 1)):
        packed = jnp.zeros((8, LANES), jnp.float32)
        for p, (f, x) in enumerate(((0, outer_x), (0, near_x), (1, near_x), (2, near_x))):
            for y in range(SIDE):
                base = (x * (SIDE * SIDE) + y * SIDE) * cap_rows + PAD + at
                value = raw[f][pl.ds(base, 8, stride=cap_rows), :]
                if f == 2:
                    value = 1.0 / (6.0 + value)
                spot = p * SIDE + y
                if side:
                    value = pltpu.roll(value, (turn + spot) & (LANES - 1), 1)
                elif spot:
                    value = pltpu.roll(value, spot, 1)
                packed = jnp.where(lane == spot, value, packed)
        ends[side] = packed

    def greeted(side):
        return pltpu.make_async_remote_copy(
            src_ref=ends.at[side], dst_ref=met.at[1 - side], send_sem=end_send.at[side],
            recv_sem=end_recv.at[side], device_id=sides[side][1], device_id_type=MESH,
        )

    for side in range(2):
        @pl.when(sides[side][0])
        def _():
            greeted(side).start()
    keep.wait()
    for copy in tallies:
        copy.wait()
    keep = pltpu.make_async_copy(every, every_s, local_sem.at[1])
    keep.start()
    keep.wait()
    before = 0
    for r in range(n):
        before = before + jnp.where(r < rank, every_s[r, 0, 0], 0)
    drift_prev = jnp.clip(before - rank * AVG, -HALF, HALF)
    drift_next = drift_prev + held - AVG
    shift = 8 * LANES - LEAD * LANES - drift_prev
    first = lax.shift_right_logical(shift, 7) - 8 + PAD
    part = shift & (LANES - 1)
    turn = (LANES - part) & (LANES - 1)
    stay = lane >= part
    low_rows, high_rows = pl.ds(0, 8), pl.ds(8, 8)
    own = pl.ds(LEAD, own_rows)
    to_left, to_right = 2, LEAD + own_rows - 8
    zero = jnp.zeros((8, LANES), jnp.float32)

    def each(fn):
        @pl.loop(0, SIDE)
        def _(x):
            @pl.loop(0, SIDE)
            def _(y):
                fn(x, y)

    def aligned(f, x, y, z, half):
        base = (x * (SIDE * SIDE) + y * SIDE + z) * cap_rows + first + 8 * half
        low, high = raw[f][pl.ds(base, 8), :], raw[f][pl.ds(base + 1, 8), :]
        return pltpu.roll(jnp.where(stay, low, high), turn, 1)

    kinds = ((out0, in0), (out1, in1), (out2, in2), (out3, in3))

    def sent(kind, side):
        return pltpu.make_async_remote_copy(
            src_ref=kinds[kind][0].at[side], dst_ref=kinds[kind][1].at[1 - side],
            send_sem=send_sem.at[2 * kind + side], recv_sem=recv_sem.at[2 * kind + side],
            device_id=sides[side][1], device_id_type=MESH,
        )

    def send(kind):
        @pl.when(has_right)
        def _():
            sent(kind, 1).start()

        @pl.when(has_left)
        def _():
            sent(kind, 0).start()

    def arrived(kind):
        @pl.when(has_left)
        def _():
            sent(kind, 1).wait_recv()

        @pl.when(has_right)
        def _():
            sent(kind, 0).wait_recv()

    def pack(put, get, planes):
        @pl.loop(0, SIDE)
        def _(x):
            for p, y in enumerate(planes):
                for z in range(SIDE):
                    put[0, p, x, z] = get(x, y, z, pl.ds(to_left, half_rows))
                    put[1, p, x, z] = get(x, y, z, pl.ds(8 + to_right, half_rows))

    outer, near_outer = (0, SIDE - 1), (0, 1, SIDE - 2, SIDE - 1)

    def step(x, y):
        for z in range(SIDE):
            wide0[x + 1, y + 1, z, low_rows, :] = aligned(0, x, y, z, 0)
            wide0[x + 1, y + 1, z, high_rows, :] = aligned(0, x, y, z, 1)
    each(step)
    pack(out0, lambda x, y, z, rows: wide0[x + 1, y + 1, z, rows, :], outer)
    send(0)

    def step(x, y):
        for z in range(SIDE):
            inverse[x, y, z, low_rows, :] = 1.0 / (aligned(2, x, y, z, 0) + 6.0)
            inverse[x, y, z, high_rows, :] = 1.0 / (aligned(2, x, y, z, 1) + 6.0)
    each(step)
    pack(out1, lambda x, y, z, rows: inverse[x, y, z, rows, :], near_outer)
    send(1)

    def step(x, y):
        for z in range(SIDE):
            source[x, y, z, low_rows, :] = aligned(1, x, y, z, 0)
            source[x, y, z, high_rows, :] = aligned(1, x, y, z, 1)
    each(step)

    for side in range(2):
        @pl.when(sides[side][0])
        def _():
            greeted(1 - side).wait_recv()
            greeted(side).wait_send()
    keep_ends = pltpu.make_async_copy(met, ghost, local_sem.at[2])
    keep_ends.start()
    keep_ends.wait()
    block = row * LANES + lane - LEAD * LANES
    for side, at, planes in (
        (0, drift_prev - 1, ((wide0, 1, SIDE - 1), (wide0, 1, SIDE), (source, 0, SIDE - 1), (inverse, 0, SIDE - 1))),
        (1, AVG + drift_next, ((wide0, 1, 2), (wide0, 1, 1), (source, 0, 0), (inverse, 0, 0))),
    ):
        here = (block == at, block + 8 * LANES == at)
        for p, (ref, off, x) in enumerate(planes):
            @pl.loop(0, SIDE)
            def _(y):
                for z in range(SIDE):
                    value = jnp.where(sides[side][0], ghost[side, z, p * SIDE + y], 0.0)
                    for half, rows in enumerate((low_rows, high_rows)):
                        old = ref[x, y + off, z, rows, :]
                        ref[x, y + off, z, rows, :] = jnp.where(here[half], value, old)

    def borders(ref):
        @pl.loop(0, SIDE)
        def _(y):
            for z in range(SIDE):
                turned = [pltpu.roll(ref[1, y + 1, z, rows, :], LANES - 1, 1) for rows in (low_rows, high_rows)]
                carry = [pltpu.roll(value, 7, 0) for value in turned]
                carry[0] = jnp.where(row == 7, carry[1], carry[0])
                for half, rows in enumerate((low_rows, high_rows)):
                    ref[SIDE + 1, y + 1, z, rows, :] = jnp.where(lane == LANES - 1, carry[half], turned[half])
                turned = [pltpu.roll(ref[SIDE, y + 1, z, rows, :], 1, 1) for rows in (low_rows, high_rows)]
                carry = [pltpu.roll(value, 1, 0) for value in turned]
                carry[1] = jnp.where(row == 0, carry[0], carry[1])
                for half, rows in enumerate((low_rows, high_rows)):
                    ref[0, y + 1, z, rows, :] = jnp.where(lane == 0, carry[half], turned[half])

        @pl.loop(0, SIDE)
        def _(x):
            for at in (0, SIDE + 1):
                ref[x + 1, at] = jnp.zeros((SIDE, WIDE, LANES), jnp.float32)

    def sweep(ref, put):
        def step(x, y):
            for rows in (low_rows, high_rows):
                line = [ref[x + 1, y + 1, z, rows, :] for z in range(SIDE)]
                for z in range(SIDE):
                    total = ref[x + 2, y + 1, z, rows, :] + ref[x, y + 1, z, rows, :]
                    total = total + (ref[x + 1, y + 2, z, rows, :] + ref[x + 1, y, z, rows, :])
                    if z + 1 < SIDE:
                        total = total + line[z + 1]
                    if z > 0:
                        total = total + line[z - 1]
                    value = (source[x, y, z, rows, :] + total) * inverse[x, y, z, rows, :]
                    put(x, y, z, rows, value)
        each(step)

    def put(x, y, z, rows, value):
        wide1[x + 1, y + 1, z, rows, :] = value
    borders(wide0)
    sweep(wide0, put)
    pack(out2, lambda x, y, z, rows: wide1[x + 1, y + 1, z, rows, :], outer)
    send(2)

    def put(x, y, z, rows, value):
        if rows is low_rows:
            result[x, y, z, pl.ds(0, 8 - LEAD), :] = value[LEAD:]
            out3[0, x, y, z] = value[to_left : to_left + half_rows]
        else:
            result[x, y, z, pl.ds(8 - LEAD, own_rows - 8 + LEAD), :] = value[:to_right]
            out3[1, x, y, z] = value[to_right : to_right + half_rows]
    borders(wide1)
    sweep(wide1, put)

    spot = lax.broadcasted_iota(jnp.int32, (half_rows, LANES), 0) * LANES
    spot = spot + lax.broadcasted_iota(jnp.int32, (half_rows, LANES), 1)
    is_left = spot < drift_prev
    is_right = spot + (AVG - HALF) >= AVG + drift_next

    def merge(kind, to, get, planes):
        got = kinds[kind][1]
        @pl.loop(0, SIDE)
        def _(x):
            for p, y in enumerate(planes):
                for z in range(SIDE):
                    mine = get(x, y, z)
                    to[p, x, z] = mine
                    to[p, x, z, pl.ds(0, half_rows), :] = jnp.where(is_left, got[0, p, x, z], mine[:half_rows])
                    to[p, x, z, pl.ds(own_rows - half_rows, half_rows), :] = jnp.where(
                        is_right, got[1, p, x, z], mine[own_rows - half_rows :]
                    )

    def faces(b):
        face, near = ((face0, near0), (face1, near1))[b]
        down = pltpu.make_async_remote_copy(
            src_ref=face.at[0], dst_ref=near.at[1], send_sem=face_send.at[2 * b],
            recv_sem=face_recv.at[2 * b], device_id=sides[2][1], device_id_type=MESH,
        )
        up = pltpu.make_async_remote_copy(
            src_ref=face.at[1], dst_ref=near.at[0], send_sem=face_send.at[2 * b + 1],
            recv_sem=face_recv.at[2 * b + 1], device_id=sides[3][1], device_id_type=MESH,
        )
        return down, up

    def send_faces(b):
        for (there, _), copy in zip(sides[2:], faces(b)):
            @pl.when(there)
            def _():
                copy.start()
        for (there, _), at in zip(sides[2:], (0, 1)):
            @pl.when(jnp.logical_not(there))
            def _():
                @pl.loop(0, SIDE)
                def _(x):
                    (near0, near1)[b][at, x] = jnp.zeros((SIDE, own_rows, LANES), jnp.float32)

    def take_faces(b):
        down, up = faces(b)
        @pl.when(has_low)
        def _():
            up.wait_recv()

        @pl.when(has_high)
        def _():
            down.wait_recv()

    arrived(0)
    merge(0, face0, lambda x, y, z: wide0[x + 1, y + 1, z, own, :], outer)
    send_faces(0)
    arrived(1)
    merge(1, inv, lambda x, y, z: inverse[x, y, z, own, :], near_outer)
    take_faces(0)

    @pl.loop(0, SIDE)
    def _(x):
        for p, at, inner in ((0, 0, 1), (1, 3, 2)):
            for z in range(SIDE):
                fix = near0[p, x, z] * inv[at, x, z]
                first_fix[p, x + 1, z] = fix
                second_fix[inner, x, z] = fix * inv[inner, x, z]

    def edges(side):
        return pltpu.make_async_remote_copy(
            src_ref=edge_out.at[side], dst_ref=edge_in.at[1 - side],
            send_sem=face_send.at[4 + side], recv_sem=face_recv.at[4 + side],
            device_id=sides[side][1], device_id_type=MESH,
        )

    for p in range(2):
        for z in range(SIDE):
            value = pltpu.roll(first_fix[p, 1, z], LANES - 1, 1)
            carry = pltpu.roll(value, own_rows - 1, 0)
            first_fix[p, SIDE + 1, z] = jnp.where(lane == LANES - 1, carry, value)
            edge_out[0, p, pl.ds(z, 1), :] = carry[own_rows - 1 : own_rows]
            value = pltpu.roll(first_fix[p, SIDE, z], 1, 1)
            carry = pltpu.roll(value, 1, 0)
            first_fix[p, 0, z] = jnp.where(lane == 0, carry, value)
            edge_out[1, p, pl.ds(z, 1), :] = carry[0:1]
    for side in range(2):
        @pl.when(sides[side][0])
        def _():
            edges(side).start()

        @pl.when(jnp.logical_not(sides[side][0]))
        def _():
            edge_in[side] = jnp.zeros((2, SIDE, LANES), jnp.float32)
    send(3)
    arrived(2)
    merge(2, face1, lambda x, y, z: wide1[x + 1, y + 1, z, own, :], outer)

    @pl.loop(0, SIDE)
    def _(x):
        for p in range(2):
            for z in range(SIDE):
                face1[p, x, z] = face1[p, x, z] + first_fix[p, x + 1, z]
    send_faces(1)
    for side in range(2):
        @pl.when(sides[side][0])
        def _():
            edges(1 - side).wait_recv()
    last_spot = (lane == LANES - 1) & (row == own_rows - 1)
    first_spot = (lane == 0) & (row == 0)
    for p in range(2):
        for z in range(SIDE):
            got = jnp.broadcast_to(edge_in[1, p, pl.ds(z, 1), :], (8, LANES))
            first_fix[p, SIDE + 1, z] = jnp.where(last_spot, got, first_fix[p, SIDE + 1, z])
            got = jnp.broadcast_to(edge_in[0, p, pl.ds(z, 1), :], (8, LANES))
            first_fix[p, 0, z] = jnp.where(first_spot, got, first_fix[p, 0, z])
    take_faces(1)

    @pl.loop(0, SIDE)
    def _(x):
        for p, at in ((0, 0), (1, 3)):
            for z in range(SIDE):
                total = near1[p, x, z] + (first_fix[p, x, z] + first_fix[p, x + 2, z])
                if z + 1 < SIDE:
                    total = total + first_fix[p, x + 1, z + 1]
                if z > 0:
                    total = total + first_fix[p, x + 1, z - 1]
                second_fix[at, x, z] = total * inv[at, x, z]

    arrived(3)
    lo, hi = pl.ds(0, half_rows), pl.ds(own_rows - half_rows, half_rows)

    def step(x, y):
        for z in range(SIDE):
            for side, rows, mask in ((0, lo, is_left), (1, hi, is_right)):
                old = result[x, y, z, rows, :]
                result[x, y, z, rows, :] = jnp.where(mask, in3[side, x, y, z], old)
    each(step)

    @pl.loop(0, SIDE)
    def _(x):
        for p, y in enumerate(near_outer):
            for z in range(SIDE):
                result[x, y, z] = result[x, y, z] + second_fix[p, x, z]
    done = pltpu.make_async_copy(result, out, out_sem)
    done.start()
    for b in range(2):
        for (there, _), copy in zip(sides[2:], faces(b)):
            @pl.when(there)
            def _():
                copy.wait_send()
    for side in range(2):
        @pl.when(sides[side][0])
        def _():
            edges(side).wait_send()
            for kind in range(4):
                sent(kind, side).wait_send()
    done.wait()


def local(state, coef, counts):
    n, groups = lax.axis_size("curve"), lax.axis_size("grp")
    cells, cap = state.shape[1], state.shape[3]
    cap_rows, own_rows, half_rows = cap // LANES, AVG // LANES, HALF // LANES
    f32 = jnp.float32
    mine = jnp.broadcast_to(counts, (1, LANES))
    vmem, hbm, smem = (pl.BlockSpec(memory_space=m) for m in (pltpu.VMEM, pl.ANY, pltpu.SMEM))
    side = (SIDE, SIDE)
    packed = [(2, 2) + side, (2, 4) + side, (2, 2) + side, (2, SIDE) + side]
    packed = [shape + (half_rows, LANES) for shape in packed]
    own = (own_rows, LANES)
    shapes = [(cells * cap_rows + 2 * PAD, LANES)] * 3
    shapes += [(SIDE + 2, SIDE + 2, SIDE, WIDE, LANES)] * 2 + [side + (SIDE, WIDE, LANES)] * 2
    shapes += packed + packed + [(2,) + side + own] * 4
    shapes += [(4,) + side + own, (2, SIDE + 2, SIDE) + own, (4,) + side + own, side + (SIDE,) + own]
    shapes += [(2, 2, SIDE, LANES)] * 2
    out = pl.pallas_call(
        functools.partial(exchange, n, groups, cap_rows),
        out_shape=jax.ShapeDtypeStruct((SIDE, SIDE, SIDE, own_rows, LANES), f32),
        in_specs=[smem, vmem, hbm, hbm],
        out_specs=hbm,
        scratch_shapes=[
            pltpu.VMEM((n, 1, LANES), jnp.int32),
            pltpu.SMEM((n, 1, LANES), jnp.int32),
            pltpu.VMEM((2, 8, LANES), f32),
            pltpu.VMEM((2, 8, LANES), f32),
            pltpu.SMEM((2, 8, LANES), f32),
        ]
        + [pltpu.VMEM(shape, f32) for shape in shapes]
        + [pltpu.SemaphoreType.DMA((k,)) for k in (n, n, 2, 2, 3, 3, 8, 8, 6, 6)]
        + [pltpu.SemaphoreType.DMA],
        compiler_params=pltpu.CompilerParams(
            collective_id=0, has_side_effects=True, vmem_limit_bytes=48 * 1024 * 1024
        ),
    )(
        counts, mine, state.reshape(2, cells * cap_rows, LANES),
        coef.reshape(cells * cap_rows, LANES),
    )
    return out.reshape(cells, 1, AVG)


def solution(mesh):
    placed = (P(None, None, "grp", "curve"), P(None, "grp", "curve"), P("grp", "curve"))
    return jax.shard_map(
        local, mesh=mesh, in_specs=placed, out_specs=P(None, "grp", "curve"), check_vma=False
    )
```
